32 devices in a mesh: dp: 4 (over y, z), sp: 8 (over x, core).
Axes of the slice: x: 4, y: 2, z: 2, core: 2. Of those that a mesh axis runs over, the one named last changes fastest.
The devices are a block of a 4x4x8 slice.
Arguments:
- hidden: bfloat16 [64, 128, 2048], P('dp', 'sp'), parts along dimension 0
- attn_norm: bfloat16 [2048], replicated
- w_q: bfloat16 [2048, 32, 64], replicated
- w_k: bfloat16 [2048, 8, 64], replicated
- w_v: bfloat16 [2048, 8, 64], replicated
- w_o: bfloat16 [32, 64, 2048], replicated
- mlp_norm: bfloat16 [2048], replicated
- w_gate: bfloat16 [2048, 8192], replicated
- w_up: bfloat16 [2048, 8192], replicated
- w_down: bfloat16 [8192, 2048], replicated
- mamba_norm: bfloat16 [2048], replicated
- w_in_x: bfloat16 [2048, 4096], replicated
- w_in_z: bfloat16 [2048, 4096], replicated
- conv_w: bfloat16 [4, 4096], replicated
- conv_b: bfloat16 [4096], replicated
- w_xproj: bfloat16 [4096, 160], replicated
- dt_norm: float32 [128], replicated
- b_norm: float32 [16], replicated
- c_norm: float32 [16], replicated
- w_dt: bfloat16 [128, 4096], replicated
- dt_bias: float32 [4096], replicated
- a_log: float32 [4096, 16], replicated
- d_skip: float32 [4096], replicated
- w_out: bfloat16 [4096, 2048], replicated
Outputs:
- output: bfloat16 [64, 128, 2048], P('dp', 'sp'), parts along dimension 0
There are 4 independent parts. The reference program is written for one: setup_inputs(seed, part) draws one part's arguments, and reference() takes and returns one part's arrays. A program takes and returns all parts, laid end to end along the dimension named above; an argument that names none is the same for every part.
All inputs are finite; a program needn't handle non-finite values.
Results may differ from the reference program's by a relative error of at most 0.02.
Values are sent between devices in bfloat16 or wider.
A program may use at most 768 MiB of HBM per device.

```python
import jax
import jax.numpy as jnp
from jax import lax

BATCH = 16
TOK_DEV = 16
SEQ = 128
D = 2048
HEADS = 32
KV_HEADS = 8
HEAD = 64
FF = 8192
INNER = 4096
STATE = 16
DT_RANK = 128
CONV = 4
EPS = 1e-6


def setup_inputs(seed: int = 0, part: int = 0) -> dict:
    key_list = jax.random.split(jax.random.key(seed), 24)
    part_key = jax.random.fold_in(key_list[0], part)

    def normal(key_idx, arr_shape, std_dev):
        return jax.random.normal(key_list[key_idx], arr_shape, jnp.float32) * std_dev

    def uniform(key_idx, arr_shape, lower_b, upper_b):
        return jax.random.uniform(key_list[key_idx], arr_shape, jnp.float32, lower_b, upper_b)

    qk_scale = 1.5 * D ** -0.5
    return {
        "hidden": jax.random.normal(part_key, (BATCH, SEQ, D), jnp.float32).astype(jnp.bfloat16),
        "attn_norm": uniform(1, (D,), 0.5, 1.5).astype(jnp.bfloat16),
        "w_q": normal(2, (D, HEADS, HEAD), qk_scale).astype(jnp.bfloat16),
        "w_k": normal(3, (D, KV_HEADS, HEAD), qk_scale).astype(jnp.bfloat16),
        "w_v": normal(4, (D, KV_HEADS, HEAD), D ** -0.5).astype(jnp.bfloat16),
        "w_o": normal(5, (HEADS, HEAD, D), (HEADS * HEAD) ** -0.5).astype(jnp.bfloat16),
        "mlp_norm": uniform(6, (D,), 0.5, 1.5).astype(jnp.bfloat16),
        "w_gate": normal(7, (D, FF), D ** -0.5).astype(jnp.bfloat16),
        "w_up": normal(8, (D, FF), D ** -0.5).astype(jnp.bfloat16),
        "w_down": normal(9, (FF, D), FF ** -0.5).astype(jnp.bfloat16),
        "mamba_norm": uniform(10, (D,), 0.5, 1.5).astype(jnp.bfloat16),
        "w_in_x": normal(11, (D, INNER), D ** -0.5).astype(jnp.bfloat16),
        "w_in_z": normal(12, (D, INNER), D ** -0.5).astype(jnp.bfloat16),
        "conv_w": normal(13, (CONV, INNER), 0.5).astype(jnp.bfloat16),
        "conv_b": normal(14, (INNER,), 0.3).astype(jnp.bfloat16),
        "w_xproj": normal(15, (INNER, DT_RANK + 2 * STATE), INNER ** -0.5).astype(jnp.bfloat16),
        "dt_norm": uniform(16, (DT_RANK,), 0.5, 1.5),
        "b_norm": uniform(17, (STATE,), 0.5, 1.5) * TOK_DEV ** 0.5,
        "c_norm": uniform(18, (STATE,), 0.5, 1.5),
        "w_dt": normal(19, (DT_RANK, INNER), DT_RANK ** -0.5).astype(jnp.bfloat16),
        "dt_bias": jnp.log(uniform(20, (INNER,), 0.25, 1.0) / TOK_DEV),
        "a_log": jnp.log(uniform(21, (INNER, STATE), 0.3, 1.5)),
        "d_skip": uniform(22, (INNER,), -1.5, 1.5),
        "w_out": normal(23, (INNER, D), INNER ** -0.5).astype(jnp.bfloat16),
    }


def rms_scale(values, gain_vec):
    values_f = values.astype(jnp.float32)
    inv_rms = lax.rsqrt(jnp.mean(values_f * values_f, axis=-1, keepdims=True) + EPS)
    return values_f * inv_rms * gain_vec.astype(jnp.float32)


def attention_layer(hidden, attn_norm, w_q, w_k, w_v, w_o):
    n_batch, seq_len, model_dim = hidden.shape
    groups = HEADS // KV_HEADS
    normed = rms_scale(hidden, attn_norm).astype(jnp.bfloat16).reshape(n_batch * seq_len, model_dim)
    queries = jnp.dot(normed, w_q.reshape(model_dim, HEADS * HEAD), preferred_element_type=jnp.float32).astype(jnp.bfloat16)
    key_proj = jnp.dot(normed, w_k.reshape(model_dim, KV_HEADS * HEAD), preferred_element_type=jnp.float32).astype(jnp.bfloat16)
    val_proj = jnp.dot(normed, w_v.reshape(model_dim, KV_HEADS * HEAD), preferred_element_type=jnp.float32).astype(jnp.bfloat16)
    queries = queries.reshape(n_batch, seq_len, KV_HEADS, groups, HEAD).transpose(2, 0, 1, 3, 4)
    key_proj = key_proj.reshape(n_batch, seq_len, KV_HEADS, HEAD).transpose(2, 0, 1, 3)
    val_proj = val_proj.reshape(n_batch, seq_len, KV_HEADS, HEAD).transpose(2, 0, 1, 3)
    causal = jnp.arange(seq_len)[:, None] >= jnp.arange(seq_len)[None, :]

    def one_group(operands):
        q_grp, k_grp, v_grp = operands
        scores = jnp.einsum("bqgd,bsd->bgqs", q_grp.astype(jnp.float32), k_grp.astype(jnp.float32)) * HEAD ** -0.5
        scores = jnp.where(causal, scores, -jnp.inf)
        attn_prob = jax.nn.softmax(scores, axis=-1).astype(jnp.bfloat16)
        return jnp.einsum("bgqs,bsd->bqgd", attn_prob.astype(jnp.float32), v_grp.astype(jnp.float32)).astype(jnp.bfloat16)

    attn_out = lax.map(one_group, (queries, key_proj, val_proj))
    attn_out = attn_out.transpose(1, 2, 0, 3, 4).reshape(n_batch * seq_len, HEADS * HEAD)
    proj_out = jnp.dot(attn_out, w_o.reshape(HEADS * HEAD, model_dim), preferred_element_type=jnp.float32)
    return (hidden.astype(jnp.float32) + proj_out.reshape(n_batch, seq_len, model_dim)).astype(jnp.bfloat16)


def mlp_layer(hidden, mlp_norm, w_gate, w_up, w_down):
    model_dim = hidden.shape[-1]
    normed = rms_scale(hidden, mlp_norm).astype(jnp.bfloat16).reshape(-1, model_dim)
    gate_pre = jnp.dot(normed, w_gate, preferred_element_type=jnp.float32)
    up_proj = jnp.dot(normed, w_up, preferred_element_type=jnp.float32)
    act_val = (jax.nn.silu(gate_pre) * up_proj).astype(jnp.bfloat16)
    down_out = jnp.dot(act_val, w_down, preferred_element_type=jnp.float32)
    return (hidden.astype(jnp.float32) + down_out.reshape(hidden.shape)).astype(jnp.bfloat16)


def mamba_mixer(hidden, mamba_norm, w_in_x, w_in_z, conv_w, conv_b, w_xproj, dt_norm, b_norm, c_norm, w_dt, dt_bias, a_log, d_skip, w_out):
    n_batch, seq_len, model_dim = hidden.shape
    normed = rms_scale(hidden, mamba_norm).astype(jnp.bfloat16).astype(jnp.float32)
    x_inner = jnp.einsum("btd,de->tbe", normed, w_in_x.astype(jnp.float32)).astype(jnp.bfloat16)
    z_gate = jnp.einsum("btd,de->tbe", normed, w_in_z.astype(jnp.float32)).astype(jnp.bfloat16)
    padded = jnp.concatenate([jnp.zeros((CONV - 1, n_batch, INNER), jnp.bfloat16), x_inner], axis=0)
    conv_acc = conv_b.astype(jnp.float32)
    for tap_idx in range(CONV):
        conv_acc = conv_acc + padded[tap_idx:tap_idx + seq_len].astype(jnp.float32) * conv_w[tap_idx].astype(jnp.float32)
    x_conv = jax.nn.silu(conv_acc).astype(jnp.bfloat16)
    x_dbl = jnp.einsum("tbe,er->tbr", x_conv.astype(jnp.float32), w_xproj.astype(jnp.float32))
    dt_in = rms_scale(x_dbl[..., :DT_RANK], dt_norm).astype(jnp.bfloat16)
    b_mat = rms_scale(x_dbl[..., DT_RANK:DT_RANK + STATE], b_norm)
    c_mat = rms_scale(x_dbl[..., DT_RANK + STATE:], c_norm)
    step_size = jax.nn.softplus(jnp.einsum("tbr,re->tbe", dt_in.astype(jnp.float32), w_dt.astype(jnp.float32)) + dt_bias)
    a_mat = -jnp.exp(a_log)

    def scan_step(ssm_state, inputs):
        step_t, x_t, b_t, c_t = inputs
        decay_t = jnp.exp(step_t[:, :, None] * a_mat)
        ssm_state = decay_t * ssm_state + (step_t * x_t.astype(jnp.float32))[:, :, None] * b_t[:, None, :]
        return ssm_state, jnp.sum(ssm_state * c_t[:, None, :], axis=-1)

    zero_state = jnp.zeros((n_batch, INNER, STATE), jnp.float32)
    y_seq = lax.scan(scan_step, zero_state, (step_size, x_conv, b_mat, c_mat))[1]
    gated_y = ((y_seq + d_skip * x_conv.astype(jnp.float32)) * jax.nn.silu(z_gate.astype(jnp.float32))).astype(jnp.bfloat16)
    mamba_out = jnp.einsum("tbe,ed->btd", gated_y.astype(jnp.float32), w_out.astype(jnp.float32))
    return (hidden.astype(jnp.float32) + mamba_out).astype(jnp.bfloat16)


def reference(hidden, attn_norm, w_q, w_k, w_v, w_o, mlp_norm, w_gate, w_up, w_down, mamba_norm, w_in_x, w_in_z, conv_w, conv_b, w_xproj, dt_norm, b_norm, c_norm, w_dt, dt_bias, a_log, d_skip, w_out):
    after_attn = attention_layer(hidden, attn_norm, w_q, w_k, w_v, w_o)
    after_mlp = mlp_layer(after_attn, mlp_norm, w_gate, w_up, w_down)
    return mamba_mixer(after_mlp, mamba_norm, w_in_x, w_in_z, conv_w, conv_b, w_xproj, dt_norm, b_norm, c_norm, w_dt, dt_bias, a_log, d_skip, w_out)
```

```python
import functools
import math

import jax
import jax.numpy as jnp
from jax import lax
from jax.experimental import pallas as pl
from jax.experimental.pallas import tpu as pltpu
from jax.sharding import PartitionSpec as P

EPS = 1e-6
CONV = 4
CH = 512
NS = 12
ST = 260
SA = 33
LOG2E = math.log2(math.e)
F32 = jnp.float32
BF16 = jnp.bfloat16


def nt_dot(a, b):
    return lax.dot_general(a, b, (((1,), (1,)), ((), ())), preferred_element_type=F32)


def nn_dot(a, b):
    return jnp.dot(a, b, preferred_element_type=F32)


def silu(v):
    return v * (1.0 / (1.0 + jnp.exp(-v)))


def softplus(v):
    return jnp.maximum(v, 0.0) + jnp.log1p(jnp.exp(-jnp.abs(v)))


def rms(v):
    return v * lax.rsqrt(jnp.mean(v * v, axis=-1, keepdims=True) + EPS)


def layer_kernel(
    hid, vecs, small, alog, wq, wk, wv, wo, wg, wu, wd, wix, wiz, wxp, wdt, wout,
    out, ring, kvw, xpw, dtw, norm, q, kv, attn, acc, act, res, xpad, conv, zg, gated, bc, dl, dc, ys, amat,
    sem, sem2,
):
    rows, dim = hid.shape
    seq = 128 if rows % 128 == 0 else rows
    n_seq = rows // seq
    inner = conv.shape[1]
    n_state = alog.shape[0]
    rank = wdt.shape[0]

    def cols(w, c, slot):
        return pltpu.make_async_copy(w.at[:, pl.ds(c * CH, CH)], ring.at[slot], sem.at[slot])

    def block(w, k, c, slot):
        return pltpu.make_async_copy(w.at[pl.ds(k * dim, dim), pl.ds(c * CH, CH)], ring.at[slot], sem.at[slot])

    def ready(slot):
        pltpu.make_async_copy(wg.at[:, pl.ds(0, CH)], ring.at[slot], sem.at[slot]).wait()

    def slot_of(p):
        return lax.rem(p + 8, NS)

    k_load = pltpu.make_async_copy(wk, kvw.at[pl.ds(0, CH)], sem2.at[0])
    v_load = pltpu.make_async_copy(wv, kvw.at[pl.ds(CH, CH)], sem2.at[1])
    xp_load = pltpu.make_async_copy(wxp, xpw, sem2.at[2])
    dt_load = pltpu.make_async_copy(wdt, dtw, sem2.at[3])
    for i in range(4):
        cols(wq, i, i).start()
    k_load.start()
    v_load.start()
    for i in range(4):
        cols(wo, i, 4 + i).start()
    cols(wg, 0, 8).start()
    cols(wu, 0, 9).start()
    cols(wg, 1, 10).start()
    cols(wu, 1, 11).start()
    xp_load.start()
    dt_load.start()

    def normalize(src, gain_row):
        gain = vecs[gain_row:gain_row + 1, :]

        def body(i, _):
            r = pl.ds(pl.multiple_of(i * 16, 16), 16)
            norm[r, :] = (rms(src[r, :].astype(F32)) * gain).astype(BF16)
            return 0

        lax.fori_loop(0, rows // 16, body, 0, unroll=2)

    for j in range(inner // 128):
        a = -jnp.exp(alog[:, j * 128:(j + 1) * 128]) * LOG2E
        amat[pl.ds(j, n_state, stride=SA), :] = a

    normalize(hid, 0)
    for i in range(4):
        ready(i)
        term = nt_dot(norm[:, i * CH:(i + 1) * CH], ring[i])
        if i == 0:
            acc[...] = term
        elif i < 3:
            acc[...] += term
        else:
            q[...] = (acc[...] + term).astype(BF16)
        if i % 2 == 0:
            cols(wg, 2 + i // 2, i).start()
        else:
            cols(wu, 2 + i // 2, i).start()
    k_load.wait()
    v_load.wait()
    kv[...] = nt_dot(norm[...], kvw[...]).astype(BF16)

    head = 64
    lane = lax.broadcasted_iota(jnp.int32, (seq, 128), 1)
    low = lane < head
    causal = (lax.rem(lax.broadcasted_iota(jnp.int32, (2 * seq, 128), 0), seq)
              >= lax.broadcasted_iota(jnp.int32, (2 * seq, 128), 1))
    pairs = CH // 128

    def spread(tile, upper):
        if upper:
            hi = jnp.where(low, 0.0, tile)
            lo = pltpu.roll(hi, head, 1)
        else:
            lo = jnp.where(low, tile, 0.0)
            hi = pltpu.roll(lo, head, 1)
        return jnp.concatenate([lo, hi], axis=0).astype(BF16)

    def attend(it, _):
        b = lax.div(it, pairs)
        m = lax.rem(it, pairs)
        r = pl.ds(pl.multiple_of(b * seq, seq), seq)
        kt = kv[r, pl.ds(pl.multiple_of(m * 128, 128), 128)].astype(F32)
        vt = kv[r, pl.ds(pl.multiple_of(CH + m * 128, 128), 128)].astype(F32)
        for par in range(2):
            k2 = spread(kt, par)
            v2 = spread(vt, par)
            c0 = pl.multiple_of((2 * m + par) * 256, 128)
            qs = jnp.concatenate([q[r, pl.ds(c0, 128)], q[r, pl.ds(c0 + 128, 128)]], axis=0)
            s = nt_dot(qs, k2)
            ps = []
            for h in range(2):
                sh = jnp.where(causal, s[:, h * 128:(h + 1) * 128] * head ** -0.5, -jnp.inf)
                e = jnp.exp(sh - jnp.max(sh, axis=-1, keepdims=True))
                ps.append((e * (1.0 / jnp.sum(e, axis=-1, keepdims=True))).astype(BF16))
            o = nn_dot(jnp.concatenate(ps, axis=1), v2).astype(BF16)
            attn[r, pl.ds(c0, 128)] = o[:seq]
            attn[r, pl.ds(c0 + 128, 128)] = o[seq:]
        return 0

    lax.fori_loop(0, n_seq * pairs, attend, 0)

    def out_proj(n, _):
        ready(4 + n)
        c = pl.ds(pl.multiple_of(n * CH, CH), CH)
        res[:, c] = (hid[:, c].astype(F32) + nn_dot(attn[...], ring[4 + n])).astype(BF16)
        block(wd, 0, n, 4 + n).start()
        return 0

    lax.fori_loop(0, 4, out_proj, 0)

    normalize(res, 1)

    def mlp(s, _):
        def up(n, _):
            sg = slot_of(2 * n)
            su = slot_of(2 * n + 1)
            ready(sg)
            ready(su)
            gate = nn_dot(norm[...], ring[sg])
            upv = nn_dot(norm[...], ring[su])
            act[:, pl.ds(pl.multiple_of(n * CH, CH), CH)] = (silu(gate) * upv).astype(BF16)

            @pl.when(s < 3)
            def _():
                cols(wg, 4 * (s + 1) + n, sg).start()
                cols(wu, 4 * (s + 1) + n, su).start()

            @pl.when(s == 3)
            def _():
                cols(wix, 2 * n, sg).start()
                cols(wix, 2 * n + 1, su).start()

            return 0

        lax.fori_loop(0, 4, up, 0)

        def down(n, _):
            sd = slot_of(8 + n)
            ready(sd)
            c = pl.ds(pl.multiple_of(n * CH, CH), CH)
            term = nn_dot(act[...], ring[sd])

            @pl.when(s == 0)
            def _():
                acc[:, c] = res[:, c].astype(F32) + term

            @pl.when((s > 0) & (s < 3))
            def _():
                acc[:, c] += term

            @pl.when(s == 3)
            def _():
                res[:, c] = (acc[:, c] + term).astype(BF16)

            @pl.when(s < 3)
            def _():
                block(wd, s + 1, n, sd).start()

            @pl.when(s == 3)
            def _():
                cols(wiz, n, sd).start()

            return 0

        lax.fori_loop(0, 4, down, 0)
        return 0

    lax.fori_loop(0, 4, mlp, 0)

    normalize(res, 2)
    pitch = seq + 8
    for b in range(n_seq):
        xpad[pl.ds(b * pitch, 8), :] = jnp.zeros((8, CH), F32)

    def inx(e, _):
        sl = slot_of(e)
        ready(sl)
        xi = nn_dot(norm[...], ring[sl]).astype(BF16).astype(F32)

        @pl.when(e < 4)
        def _():
            cols(wiz, 4 + e, sl).start()

        @pl.when(e >= 4)
        def _():
            block(wout, lax.rem(e, 2), lax.div(e - 4, 2), sl).start()

        half = lax.div(e, 4)
        c_in = pl.ds(pl.multiple_of(lax.rem(e, 4) * CH, CH), CH)
        bias = vecs[pl.ds(3 + half, 1), c_in]
        taps = [vecs[pl.ds(9 + 2 * j + half, 1), c_in] for j in range(CONV)]
        c = pl.ds(pl.multiple_of(e * CH, CH), CH)
        for b in range(n_seq):
            xpad[pl.ds(b * pitch + 8, seq), :] = xi[b * seq:(b + 1) * seq]
        for b in range(n_seq):
            v = bias
            for j in range(CONV):
                v = v + xpad[pl.ds(b * pitch + 8 - (CONV - 1) + j, seq), :] * taps[j]
            conv[pl.ds(b * seq, seq), c] = silu(v).astype(BF16)
        return 0

    lax.fori_loop(0, 8, inx, 0)

    xp_load.wait()
    dt_load.wait()
    r = nt_dot(conv[...], xpw[...])
    dt_in = (rms(r[:, :rank]) * small[:, :rank]).astype(BF16)
    bm = rms(r[:, rank:rank + n_state]) * small[:, rank:rank + n_state]
    cm = rms(r[:, rank + n_state:rank + 2 * n_state]) * small[:, rank + n_state:rank + 2 * n_state]
    for n in range(n_state):
        bc[n] = jnp.broadcast_to(bm[:, n:n + 1], (rows, 128))
        bc[n_state + n] = jnp.broadcast_to(cm[:, n:n + 1], (rows, 128))

    def inz(e, _):
        sl = slot_of(8 + e)
        ready(sl)
        zg[:, pl.ds(pl.multiple_of(e * CH, CH), CH)] = nn_dot(norm[...], ring[sl]).astype(BF16)

        @pl.when(e < 4)
        def _():
            block(wout, lax.rem(e, 2), 2 + lax.div(e, 2), sl).start()

        return 0

    lax.fori_loop(0, 8, inz, 0)

    for blk in range(inner // 1024):
        for j in range(8):
            c0 = blk * 1024 + j * 128
            pre = nn_dot(dt_in, dtw[:, c0:c0 + 128]) + vecs[5 + c0 // 2048:6 + c0 // 2048, c0 % 2048:c0 % 2048 + 128]
            step = softplus(pre)
            dl[pl.ds(j * ST, rows), :] = step
            dc[pl.ds(j * ST, rows), :] = step * conv[:, c0:c0 + 128].astype(F32)
        a_rows = [amat[pl.ds(n * SA + blk * 8, 8), :] for n in range(n_state)]

        def one_seq(b, _):
            def step_fn(t, hs):
                row = b * seq + t
                d = dl[pl.ds(row, 8, stride=ST), :]
                x = dc[pl.ds(row, 8, stride=ST), :]
                new = []
                y = None
                for n in range(n_state):
                    bv = jnp.broadcast_to(bc[n, pl.ds(row, 1), :], (8, 128))
                    cv = jnp.broadcast_to(bc[n_state + n, pl.ds(row, 1), :], (8, 128))
                    hn = jnp.exp2(d * a_rows[n]) * hs[n] + x * bv
                    new.append(hn)
                    y = hn * cv if y is None else y + hn * cv
                ys[pl.ds(row, 8, stride=ST), :] = y
                return tuple(new)

            lax.fori_loop(0, seq, step_fn, tuple(jnp.zeros((8, 128), F32) for _ in range(n_state)), unroll=4)
            return 0

        lax.fori_loop(0, n_seq, one_seq, 0)
        for j in range(8):
            c0 = blk * 1024 + j * 128
            skip = vecs[7 + c0 // 2048:8 + c0 // 2048, c0 % 2048:c0 % 2048 + 128]
            y = ys[pl.ds(j * ST, rows), :] + skip * conv[:, c0:c0 + 128].astype(F32)
            gated[:, c0:c0 + 128] = (y * silu(zg[:, c0:c0 + 128].astype(F32))).astype(BF16)

    def final(n, _):
        s0 = slot_of(4 + 2 * n)
        s1 = slot_of(5 + 2 * n)
        ready(s0)
        ready(s1)
        c = pl.ds(pl.multiple_of(n * CH, CH), CH)
        y = nn_dot(gated[:, :dim], ring[s0]) + nn_dot(gated[:, dim:], ring[s1])
        out[:, c] = (res[:, c].astype(F32) + y).astype(BF16)
        return 0

    lax.fori_loop(0, 4, final, 0)


def local_layers(hid, attn_norm, w_q, w_k, w_v, w_o, mlp_norm, w_gate, w_up, w_down, mamba_norm, w_in_x, w_in_z,
                 conv_w, conv_b, w_xproj, dt_norm, b_norm, c_norm, w_dt, dt_bias, a_log, d_skip, w_out):
    rows, dim = hid.shape
    inner, n_state = a_log.shape
    rank = w_dt.shape[0]
    flat = [v.astype(F32).reshape(-1) for v in (attn_norm, mlp_norm, mamba_norm, conv_b, dt_bias, d_skip, conv_w)]
    vecs = jnp.concatenate(flat).reshape(-1, dim)
    small = jnp.concatenate([dt_norm, b_norm, c_norm]).reshape(1, -1)
    wq_t = w_q.transpose(1, 2, 0).reshape(-1, dim)
    wk_t = w_k.transpose(1, 2, 0).reshape(-1, dim)
    wv_t = w_v.transpose(1, 2, 0).reshape(-1, dim)
    kv_dim = wk_t.shape[0]
    wo = w_o.reshape(-1, dim)
    wxp = w_xproj.T
    vm = pl.BlockSpec(memory_space=pltpu.VMEM)
    hbm = pl.BlockSpec(memory_space=pl.ANY)
    return pl.pallas_call(
        layer_kernel,
        out_shape=jax.ShapeDtypeStruct((rows, dim), BF16),
        in_specs=[vm] * 4 + [hbm] * 12,
        out_specs=vm,
        scratch_shapes=[
            pltpu.VMEM((NS, dim, CH), BF16),
            pltpu.VMEM((2 * kv_dim, dim), BF16),
            pltpu.VMEM(wxp.shape, BF16),
            pltpu.VMEM(w_dt.shape, BF16),
            pltpu.VMEM((rows, dim), BF16),
            pltpu.VMEM((rows, dim), BF16),
            pltpu.VMEM((rows, 2 * kv_dim), BF16),
            pltpu.VMEM((rows, dim), BF16),
            pltpu.VMEM((rows, dim), F32),
            pltpu.VMEM((rows, dim), BF16),
            pltpu.VMEM((rows, dim), BF16),
            pltpu.VMEM((rows + 8 * (rows // 128), CH), F32),
            pltpu.VMEM((rows, inner), BF16),
            pltpu.VMEM((rows, inner), BF16),
            pltpu.VMEM((rows, inner), BF16),
            pltpu.VMEM((2 * n_state, rows, 128), F32),
            pltpu.VMEM((8 * ST, 128), F32),
            pltpu.VMEM((8 * ST, 128), F32),
            pltpu.VMEM((8 * ST, 128), F32),
            pltpu.VMEM((n_state * SA, 128), F32),
            pltpu.SemaphoreType.DMA((NS,)),
            pltpu.SemaphoreType.DMA((4,)),
        ],
        compiler_params=pltpu.CompilerParams(vmem_limit_bytes=63 * 1024 * 1024),
        cost_estimate=pl.CostEstimate(flops=45_000_000_000, bytes_accessed=180_000_000, transcendentals=20_000_000),
        name="layers",
    )(hid, vecs, small, a_log.T, wq_t, wk_t, wv_t, wo, w_gate, w_up, w_down, w_in_x, w_in_z, wxp, w_dt, w_out)


def group_layers(hidden, *weights, n_shards):
    n_batch, tok, dim = hidden.shape
    per = n_batch // n_shards
    seq = lax.all_to_all(hidden.reshape(n_shards, per, tok, dim), "sp", 0, 0)
    seq = seq.transpose(1, 0, 2, 3).reshape(per * n_shards * tok, dim)
    done = local_layers(seq, *weights)
    done = done.reshape(per, n_shards, tok, dim).transpose(1, 0, 2, 3)
    return lax.all_to_all(done, "sp", 0, 0).reshape(n_batch, tok, dim)


def solution(mesh):
    act_spec = P("dp", "sp", None)
    return jax.shard_map(
        functools.partial(group_layers, n_shards=mesh.shape["sp"]),
        mesh=mesh,
        in_specs=(act_spec,) + (P(),) * 23,
        out_specs=act_spec,
        check_vma=False,
    )
```

```python
import functools
import math

import jax
import jax.numpy as jnp
from jax import lax
from jax.experimental import pallas as pl
from jax.experimental.pallas import tpu as pltpu
from jax.sharding import PartitionSpec as P

EPS = 1e-6
CONV = 4
CH = 512
NS = 12
ST = 260
SA = 33
LOG2E = math.log2(math.e)
F32 = jnp.float32
BF16 = jnp.bfloat16


def nt_dot(a, b):
    return lax.dot_general(a, b, (((1,), (1,)), ((), ())), preferred_element_type=F32)


def nn_dot(a, b):
    return jnp.dot(a, b, preferred_element_type=F32)


def silu(v):
    return v * (1.0 / (1.0 + jnp.exp(-v)))


def softplus(v):
    return jnp.maximum(v, 0.0) + jnp.log1p(jnp.exp(-jnp.abs(v)))


def rms(v):
    return v * lax.rsqrt(jnp.mean(v * v, axis=-1, keepdims=True) + EPS)


def layer_kernel(
    n_dev, axis, x_in, attn_norm, mlp_norm, mamba_norm, conv_w, conv_b, dt_norm, b_norm, c_norm, dt_bias, d_skip, alog,
    wq, wk, wv, wo, wg, wu, wd, wix, wiz, wxp, wdt, wout,
    out, ring, kvw, xpw, dtw, hid, norm, q, kv, acc, res, xpad, conv, zg, bc, dl, dc, ys, amat,
    sem, sem2, in_send, in_recv, out_send, out_recv, own_sem,
):
    n_batch, tok, dim = x_in.shape
    per = n_batch // n_dev
    seq = tok * n_dev
    rows = per * seq
    inner = conv.shape[1]
    n_state = alog.shape[0]
    rank = wdt.shape[0]
    me = lax.axis_index(axis) if n_dev > 1 else 0
    act = q

    def peer_of(k):
        chips = n_dev // 2
        chip = lax.rem(lax.div(me, 2) + k // 2, chips)
        return chip * 2 + lax.rem(lax.rem(me, 2) + k % 2, 2)

    order = sorted(range(1, n_dev), key=lambda k: (-min(k // 2, n_dev // 2 - k // 2), k % 2, k))

    def cols(w, c, slot):
        return pltpu.make_async_copy(w.at[:, pl.ds(c * CH, CH)], ring.at[slot], sem.at[slot])

    def block(w, k, c, slot):
        return pltpu.make_async_copy(w.at[pl.ds(k * dim, dim), pl.ds(c * CH, CH)], ring.at[slot], sem.at[slot])

    def ready(slot):
        pltpu.make_async_copy(wg.at[:, pl.ds(0, CH)], ring.at[slot], sem.at[slot]).wait()

    def slot_of(p):
        return lax.rem(p + 8, NS)

    def send_in(k, b):
        to = peer_of(k)
        return pltpu.make_async_remote_copy(
            src_ref=x_in.at[to * per + b],
            dst_ref=hid.at[pl.ds(pl.multiple_of(b * seq + me * tok, tok), tok)],
            send_sem=in_send.at[k - 1, b],
            recv_sem=in_recv.at[k - 1, b],
            device_id={axis: to},
            device_id_type=pl.DeviceIdType.MESH,
        )

    own_in = [
        pltpu.make_async_copy(
            x_in.at[me * per + b],
            hid.at[pl.ds(pl.multiple_of(b * seq + me * tok, tok), tok)],
            own_sem.at[b, dim // CH],
        )
        for b in range(per)
    ]

    k_load = pltpu.make_async_copy(wk, kvw.at[pl.ds(0, CH)], sem2.at[0])
    v_load = pltpu.make_async_copy(wv, kvw.at[pl.ds(CH, CH)], sem2.at[1])
    xp_load = pltpu.make_async_copy(wxp, xpw, sem2.at[2])
    dt_load = pltpu.make_async_copy(wdt, dtw, sem2.at[3])
    for copy in own_in:
        copy.start()
    if n_dev > 1:
        barrier = pltpu.get_barrier_semaphore()
        for k in range(1, n_dev):
            pl.semaphore_signal(barrier, inc=1, device_id={axis: peer_of(k)}, device_id_type=pl.DeviceIdType.MESH)
    for i in range(4):
        cols(wq, i, i).start()
    k_load.start()
    v_load.start()
    if n_dev > 1:
        pl.semaphore_wait(barrier, n_dev - 1)
        for b in range(per):
            for k in order:
                send_in(k, b).start()
    for i in range(4):
        cols(wo, i, 4 + i).start()
    cols(wg, 0, 8).start()
    cols(wu, 0, 9).start()
    cols(wg, 1, 10).start()
    cols(wu, 1, 11).start()
    xp_load.start()
    dt_load.start()

    def normalize(src, gain_ref, start=0, count=rows):
        gain = gain_ref[...].astype(F32).reshape(1, dim)

        def body(i, _):
            r = pl.ds(pl.multiple_of(start + i * 16, 16), 16)
            norm[r, :] = (rms(src[r, :].astype(F32)) * gain).astype(BF16)
            return 0

        lax.fori_loop(0, count // 16, body, 0, unroll=2)

    for j in range(inner // 128):
        a = -jnp.exp(alog[:, j * 128:(j + 1) * 128]) * LOG2E
        amat[pl.ds(j, n_state, stride=SA), :] = a

    head = 64
    lane = lax.broadcasted_iota(jnp.int32, (seq, 128), 1)
    low = lane < head
    causal = (lax.rem(lax.broadcasted_iota(jnp.int32, (2 * seq, 128), 0), seq)
              >= lax.broadcasted_iota(jnp.int32, (2 * seq, 128), 1))
    pairs = CH // 128

    def spread(tile, upper):
        if upper:
            hi = jnp.where(low, 0.0, tile)
            lo = pltpu.roll(hi, head, 1)
        else:
            lo = jnp.where(low, tile, 0.0)
            hi = pltpu.roll(lo, head, 1)
        return jnp.concatenate([lo, hi], axis=0).astype(BF16)

    for b in range(per):
        own_in[b].wait()
        if n_dev > 1:
            for k in order:
                send_in(k, b).wait_recv()
        rb = pl.ds(b * seq, seq)
        normalize(hid, attn_norm, b * seq, seq)
        for i in range(4):
            if b == 0:
                ready(i)
            term = nt_dot(norm[rb, i * CH:(i + 1) * CH], ring[i])
            if i == 0:
                acc[rb, :] = term
            elif i < 3:
                acc[rb, :] += term
            else:
                q[rb, :] = (acc[rb, :] + term).astype(BF16)
            if b == per - 1:
                if i % 2 == 0:
                    cols(wg, 2 + i // 2, i).start()
                else:
                    cols(wu, 2 + i // 2, i).start()
        if b == 0:
            k_load.wait()
            v_load.wait()
        kv[rb, :] = nt_dot(norm[rb, :], kvw[...]).astype(BF16)

        def attend(m, _, rb=rb):
            kt = kv[rb, pl.ds(pl.multiple_of(m * 128, 128), 128)].astype(F32)
            vt = kv[rb, pl.ds(pl.multiple_of(CH + m * 128, 128), 128)].astype(F32)
            for par in range(2):
                k2 = spread(kt, par)
                v2 = spread(vt, par)
                c0 = pl.multiple_of((2 * m + par) * 256, 128)
                qs = jnp.concatenate([q[rb, pl.ds(c0, 128)], q[rb, pl.ds(c0 + 128, 128)]], axis=0)
                s = nt_dot(qs, k2)
                ps = []
                for h in range(2):
                    sh = jnp.where(causal, s[:, h * 128:(h + 1) * 128] * head ** -0.5, -jnp.inf)
                    e = jnp.exp(sh - jnp.max(sh, axis=-1, keepdims=True))
                    ps.append((e * (1.0 / jnp.sum(e, axis=-1, keepdims=True))).astype(BF16))
                o = nn_dot(jnp.concatenate(ps, axis=1), v2).astype(BF16)
                norm[rb, pl.ds(c0, 128)] = o[:seq]
                norm[rb, pl.ds(c0 + 128, 128)] = o[seq:]
            return 0

        lax.fori_loop(0, pairs, attend, 0)

    def out_proj(n, _):
        ready(4 + n)
        c = pl.ds(pl.multiple_of(n * CH, CH), CH)
        res[:, c] = (hid[:, c].astype(F32) + nn_dot(norm[...], ring[4 + n])).astype(BF16)
        block(wd, 0, n, 4 + n).start()
        return 0

    lax.fori_loop(0, 4, out_proj, 0)

    normalize(res, mlp_norm)

    def mlp(s, _):
        def up(n, _):
            sg = slot_of(2 * n)
            su = slot_of(2 * n + 1)
            ready(sg)
            ready(su)
            gate = nn_dot(norm[...], ring[sg])
            upv = nn_dot(norm[...], ring[su])
            act[:, pl.ds(pl.multiple_of(n * CH, CH), CH)] = (silu(gate) * upv).astype(BF16)

            @pl.when(s < 3)
            def _():
                cols(wg, 4 * (s + 1) + n, sg).start()
                cols(wu, 4 * (s + 1) + n, su).start()

            @pl.when(s == 3)
            def _():
                cols(wix, 2 * n, sg).start()
                cols(wix, 2 * n + 1, su).start()

            return 0

        lax.fori_loop(0, 4, up, 0)

        def down(n, _):
            sd = slot_of(8 + n)
            ready(sd)
            c = pl.ds(pl.multiple_of(n * CH, CH), CH)
            term = nn_dot(act[...], ring[sd])

            @pl.when(s == 0)
            def _():
                acc[:, c] = res[:, c].astype(F32) + term

            @pl.when((s > 0) & (s < 3))
            def _():
                acc[:, c] += term

            @pl.when(s == 3)
            def _():
                res[:, c] = (acc[:, c] + term).astype(BF16)

            @pl.when(s < 3)
            def _():
                block(wd, s + 1, n, sd).start()

            @pl.when(s == 3)
            def _():
                cols(wiz, n, sd).start()

            return 0

        lax.fori_loop(0, 4, down, 0)
        return 0

    lax.fori_loop(0, 4, mlp, 0)

    normalize(res, mamba_norm)
    pitch = seq + 8
    for i in range(2):
        for b in range(per):
            xpad[i, pl.ds(b * pitch, 8), :] = jnp.zeros((8, CH), F32)

    def conv_chunk(e):
        i = lax.rem(e, 2)
        c = pl.ds(pl.multiple_of(e * CH, CH), CH)
        bias = conv_b[c].astype(F32).reshape(1, CH)
        taps = [conv_w[j:j + 1, c].astype(F32) for j in range(CONV)]
        for b in range(per):
            v = bias
            for j in range(CONV):
                v = v + xpad[i, pl.ds(b * pitch + 8 - (CONV - 1) + j, seq), :] * taps[j]
            conv[pl.ds(b * seq, seq), c] = silu(v).astype(BF16)

    def inx(e, _):
        sl = slot_of(e)
        ready(sl)
        conv_chunk(jnp.maximum(e - 1, 0))
        xi = nn_dot(norm[...], ring[sl]).astype(BF16).astype(F32)
        for b in range(per):
            xpad[lax.rem(e, 2), pl.ds(b * pitch + 8, seq), :] = xi[b * seq:(b + 1) * seq]

        @pl.when(e < 4)
        def _():
            cols(wiz, 4 + e, sl).start()

        @pl.when(e >= 4)
        def _():
            block(wout, lax.rem(e, 2), lax.div(e - 4, 2), sl).start()

        return 0

    lax.fori_loop(0, inner // CH, inx, 0)
    conv_chunk(jnp.int32(inner // CH - 1))

    xp_load.wait()
    dt_load.wait()
    r = nt_dot(conv[...], xpw[...])
    dt_in = (rms(r[:, :rank]) * dt_norm[...].reshape(1, rank)).astype(BF16)
    bm = rms(r[:, rank:rank + n_state]) * b_norm[...].reshape(1, n_state)
    cm = rms(r[:, rank + n_state:rank + 2 * n_state]) * c_norm[...].reshape(1, n_state)
    for n in range(n_state):
        bc[n] = jnp.broadcast_to(bm[:, n:n + 1], (rows, 128))
        bc[n_state + n] = jnp.broadcast_to(cm[:, n:n + 1], (rows, 128))
    kv[:, :rank] = dt_in

    def inz(e, _):
        sl = slot_of(8 + e)
        ready(sl)
        c = pl.ds(pl.multiple_of(e * CH, CH), CH)
        step = softplus(nn_dot(kv[:, :rank], dtw[:, c]) + dt_bias[c].reshape(1, CH))
        prod = step * conv[:, c].astype(F32)
        for j in range(CH // 128):
            at = pl.ds((e * (CH // 128) + j) * ST, rows)
            dl[at, :] = step[:, j * 128:(j + 1) * 128]
            dc[at, :] = prod[:, j * 128:(j + 1) * 128]
        zg[:, c] = nn_dot(norm[...], ring[sl]).astype(BF16)

        @pl.when(e < 4)
        def _():
            block(wout, lax.rem(e, 2), 2 + lax.div(e, 2), sl).start()

        return 0

    lax.fori_loop(0, inner // CH, inz, 0)

    def send_out(k, b, n):
        to = peer_of(k)
        return pltpu.make_async_remote_copy(
            src_ref=q.at[pl.ds(pl.multiple_of(b * seq + to * tok, tok), tok), pl.ds(n * CH, CH)],
            dst_ref=out.at[me * per + b, :, pl.ds(n * CH, CH)],
            send_sem=out_send,
            recv_sem=out_recv,
            device_id={axis: to},
            device_id_type=pl.DeviceIdType.MESH,
        )

    def own_out(b, n):
        return pltpu.make_async_copy(
            q.at[pl.ds(pl.multiple_of(b * seq + me * tok, tok), tok), pl.ds(n * CH, CH)],
            out.at[me * per + b, :, pl.ds(n * CH, CH)],
            own_sem.at[b, n],
        )

    for b in range(per):
        rb = pl.ds(b * seq, seq)

        def scan_block(blk, _, b=b, rb=rb):
            base = blk * (8 * ST) + b * seq
            a_rows = [amat[pl.ds(n * SA + blk * 8, 8), :] for n in range(n_state)]

            def step_fn(t, hs):
                at = pl.ds(base + t, 8, stride=ST)
                d = dl[at, :]
                x = dc[at, :]
                new = []
                y = None
                for n in range(n_state):
                    bv = jnp.broadcast_to(bc[n, pl.ds(b * seq + t, 1), :], (8, 128))
                    cv = jnp.broadcast_to(bc[n_state + n, pl.ds(b * seq + t, 1), :], (8, 128))
                    hn = jnp.exp2(d * a_rows[n]) * hs[n] + x * bv
                    new.append(hn)
                    y = hn * cv if y is None else y + hn * cv
                ys[pl.ds(t, 8, stride=seq + 4), :] = y
                return tuple(new)

            lax.fori_loop(0, seq, step_fn, tuple(jnp.zeros((8, 128), F32) for _ in range(n_state)), unroll=4)
            for j in range(8):
                c = pl.ds(pl.multiple_of(blk * 1024 + j * 128, 128), 128)
                y = ys[pl.ds(j * (seq + 4), seq), :] + d_skip[c].reshape(1, 128) * conv[rb, c].astype(F32)
                zg[rb, c] = (y * silu(zg[rb, c].astype(F32))).astype(BF16)
            return 0

        lax.fori_loop(0, inner // 1024, scan_block, 0)

        for n in range(dim // CH):
            s0 = (4 + 2 * n + 8) % NS
            s1 = (5 + 2 * n + 8) % NS
            if b == 0:
                ready(s0)
                ready(s1)
            c = slice(n * CH, (n + 1) * CH)
            y = nn_dot(zg[rb, :dim], ring[s0]) + nn_dot(zg[rb, dim:], ring[s1])
            q[rb, c] = (res[rb, c].astype(F32) + y).astype(BF16)
            own_out(b, n).start()
            if n_dev > 1:
                for k in order:
                    send_out(k, b, n).start()

    for b in range(per):
        for n in range(dim // CH):
            own_out(b, n).wait()
    if n_dev > 1:
        for b in range(per):
            for k in order:
                send_in(k, b).wait_send()
        everything = pltpu.make_async_remote_copy(
            src_ref=out.at[pl.ds(0, n_batch - per)],
            dst_ref=out.at[pl.ds(0, n_batch - per)],
            send_sem=out_send,
            recv_sem=out_recv,
            device_id={axis: peer_of(1)},
            device_id_type=pl.DeviceIdType.MESH,
        )
        everything.wait_send()
        everything.wait_recv()


def local_layers(n_dev, axis, hidden, attn_norm, w_q, w_k, w_v, w_o, mlp_norm, w_gate, w_up, w_down, mamba_norm,
                 w_in_x, w_in_z, conv_w, conv_b, w_xproj, dt_norm, b_norm, c_norm, w_dt, dt_bias, a_log, d_skip, w_out):
    n_batch, tok, dim = hidden.shape
    rows = n_batch * tok
    inner, n_state = a_log.shape
    wq_t = w_q.transpose(1, 2, 0).reshape(-1, dim)
    wk_t = w_k.transpose(1, 2, 0).reshape(-1, dim)
    wv_t = w_v.transpose(1, 2, 0).reshape(-1, dim)
    kv_dim = wk_t.shape[0]
    wo = w_o.reshape(-1, dim)
    wxp = w_xproj.T
    vm = pl.BlockSpec(memory_space=pltpu.VMEM)
    hbm = pl.BlockSpec(memory_space=pl.ANY)
    peers = max(n_dev - 1, 1)
    per = n_batch // n_dev
    lanes = inner // 128
    params = dict(vmem_limit_bytes=63 * 1024 * 1024)
    if n_dev > 1:
        params.update(collective_id=0, has_side_effects=True)
    return pl.pallas_call(
        functools.partial(layer_kernel, n_dev, axis),
        out_shape=jax.ShapeDtypeStruct(hidden.shape, BF16),
        in_specs=[hbm] + [vm] * 11 + [hbm] * 12,
        out_specs=hbm,
        scratch_shapes=[
            pltpu.VMEM((NS, dim, CH), BF16),
            pltpu.VMEM((2 * kv_dim, dim), BF16),
            pltpu.VMEM(wxp.shape, BF16),
            pltpu.VMEM(w_dt.shape, BF16),
            pltpu.VMEM((rows, dim), BF16),
            pltpu.VMEM((rows, dim), BF16),
            pltpu.VMEM((rows, dim), BF16),
            pltpu.VMEM((rows, 2 * kv_dim), BF16),
            pltpu.VMEM((rows, dim), F32),
            pltpu.VMEM((rows, dim), BF16),
            pltpu.VMEM((2, rows + 8 * per, CH), F32),
            pltpu.VMEM((rows, inner), BF16),
            pltpu.VMEM((rows, inner), BF16),
            pltpu.VMEM((2 * n_state, rows, 128), F32),
            pltpu.VMEM((lanes * ST, 128), F32),
            pltpu.VMEM((lanes * ST, 128), F32),
            pltpu.VMEM((8 * (rows // per + 4), 128), F32),
            pltpu.VMEM((n_state * SA, 128), F32),
            pltpu.SemaphoreType.DMA((NS,)),
            pltpu.SemaphoreType.DMA((4,)),
            pltpu.SemaphoreType.DMA((peers, per)),
            pltpu.SemaphoreType.DMA((peers, per)),
            pltpu.SemaphoreType.DMA,
            pltpu.SemaphoreType.DMA,
            pltpu.SemaphoreType.DMA((per, dim // CH + 1)),
        ],
        compiler_params=pltpu.CompilerParams(**params),
        cost_estimate=pl.CostEstimate(flops=45_000_000_000, bytes_accessed=180_000_000, transcendentals=20_000_000),
        name="layers",
    )(hidden, attn_norm, mlp_norm, mamba_norm, conv_w, conv_b, dt_norm, b_norm, c_norm, dt_bias, d_skip, a_log.T,
      wq_t, wk_t, wv_t, wo, w_gate, w_up, w_down, w_in_x, w_in_z, wxp, w_dt, w_out)


def solution(mesh):
    act_spec = P("dp", "sp", None)
    return jax.shard_map(
        functools.partial(local_layers, mesh.shape["sp"], "sp"),
        mesh=mesh,
        in_specs=(act_spec,) + (P(),) * 23,
        out_specs=act_spec,
        check_vma=False,
    )
```

```python
import functools
import math

import jax
import jax.numpy as jnp
from jax import lax
from jax.experimental import pallas as pl
from jax.experimental.pallas import tpu as pltpu
from jax.sharding import PartitionSpec as P

EPS = 1e-6
CONV = 4
CH = 512
NS = 12
ST = 260
SA = 33
LOG2E = math.log2(math.e)
F32 = jnp.float32
BF16 = jnp.bfloat16


def nt_dot(a, b):
    return lax.dot_general(a, b, (((1,), (1,)), ((), ())), preferred_element_type=F32)


def nn_dot(a, b):
    return jnp.dot(a, b, preferred_element_type=F32)


def silu(v):
    return v * (1.0 / (1.0 + jnp.exp(-v)))


def softplus(v):
    return jnp.maximum(v, 0.0) + jnp.log1p(jnp.exp(-jnp.abs(v)))


def rms(v):
    return v * lax.rsqrt(jnp.mean(v * v, axis=-1, keepdims=True) + EPS)


def layer_kernel(
    n_dev, axis, x_in, attn_norm, mlp_norm, mamba_norm, conv_w, conv_b, dt_norm, b_norm, c_norm, dt_bias, d_skip, alog,
    wq, wk, wv, wo, wg, wu, wd, wix, wiz, wxp, wdt, wout,
    out, ring, kvw, xpw, dtw, hid, norm, q, kv, acc, res, xpad, conv, zg, bc, dl, dc, ys, amat,
    spare, sem, sem2, sem3, in_send, in_recv, out_send, out_recv, own_sem,
):
    n_batch, tok, dim = x_in.shape
    per = n_batch // n_dev
    seq = tok * n_dev
    rows = per * seq
    inner = wix.shape[1]
    chunks = inner // CH
    n_state = alog.shape[0]
    rank = wdt.shape[0]
    me = lax.axis_index(axis) if n_dev > 1 else 0
    act = q

    def peer_of(k):
        chips = n_dev // 2
        chip = lax.rem(lax.div(me, 2) + k // 2, chips)
        return chip * 2 + lax.rem(lax.rem(me, 2) + k % 2, 2)

    order = sorted(range(1, n_dev), key=lambda k: (-min(k // 2, n_dev // 2 - k // 2), k % 2, k))

    def cols(w, c, slot):
        return pltpu.make_async_copy(w.at[:, pl.ds(c * CH, CH)], ring.at[slot], sem.at[slot])

    def block(w, k, c, slot):
        return pltpu.make_async_copy(w.at[pl.ds(k * dim, dim), pl.ds(c * CH, CH)], ring.at[slot], sem.at[slot])

    early = [spare.at[0], spare.at[1], conv, zg]

    def first_down(n):
        return pltpu.make_async_copy(wd.at[pl.ds(0, dim), pl.ds(n * CH, CH)], early[n], sem3.at[n])

    def piece(e, b):
        return pl.ds(pl.multiple_of(e * rows + b * seq, seq), seq)

    def ready(slot):
        pltpu.make_async_copy(wg.at[:, pl.ds(0, CH)], ring.at[slot], sem.at[slot]).wait()

    def slot_of(p):
        return lax.rem(p + 8, NS)

    def send_in(k, b):
        to = peer_of(k)
        return pltpu.make_async_remote_copy(
            src_ref=x_in.at[to * per + b],
            dst_ref=hid.at[pl.ds(pl.multiple_of(b * seq + me * tok, tok), tok)],
            send_sem=in_send.at[k - 1, b],
            recv_sem=in_recv.at[k - 1, b],
            device_id={axis: to},
            device_id_type=pl.DeviceIdType.MESH,
        )

    own_in = [
        pltpu.make_async_copy(
            x_in.at[me * per + b],
            hid.at[pl.ds(pl.multiple_of(b * seq + me * tok, tok), tok)],
            own_sem.at[b, dim // CH],
        )
        for b in range(per)
    ]

    k_load = pltpu.make_async_copy(wk, kvw.at[pl.ds(0, CH)], sem2.at[0])
    v_load = pltpu.make_async_copy(wv, kvw.at[pl.ds(CH, CH)], sem2.at[1])
    xp_load = pltpu.make_async_copy(wxp, xpw, sem2.at[2])
    dt_load = pltpu.make_async_copy(wdt, dtw, sem2.at[3])
    for copy in own_in:
        copy.start()
    if n_dev > 1:
        barrier = pltpu.get_barrier_semaphore()
        for k in range(1, n_dev):
            pl.semaphore_signal(barrier, inc=1, device_id={axis: peer_of(k)}, device_id_type=pl.DeviceIdType.MESH)
    for i in range(4):
        cols(wq, i, i).start()
    k_load.start()
    v_load.start()
    if n_dev > 1:
        pl.semaphore_wait(barrier, n_dev - 1)
        for b in range(per):
            for k in order:
                send_in(k, b).start()
    for i in range(4):
        cols(wo, i, 4 + i).start()
    cols(wg, 0, 8).start()
    cols(wu, 0, 9).start()
    cols(wg, 1, 10).start()
    cols(wu, 1, 11).start()
    for n in range(4):
        first_down(n).start()
    xp_load.start()
    dt_load.start()

    def normalize(src, gain_ref, start=0, count=rows, keep=None):
        gain = gain_ref[...].astype(F32).reshape(1, dim)

        def body(i, _):
            r = pl.ds(pl.multiple_of(start + i * 16, 16), 16)
            v = src[r, :]
            if keep is not None:
                v = v.astype(BF16)
                keep[r, :] = v
            v = v.astype(F32)
            if keep is not None:
                src[r, :] = v
            norm[r, :] = (rms(v) * gain).astype(BF16)
            return 0

        lax.fori_loop(0, count // 16, body, 0, unroll=2)

    for j in range(inner // 128):
        a = -jnp.exp(alog[:, j * 128:(j + 1) * 128]) * LOG2E
        amat[pl.ds(j, n_state, stride=SA), :] = a

    head = 64
    lane = lax.broadcasted_iota(jnp.int32, (seq, 128), 1)
    low = lane < head
    causal = (lax.rem(lax.broadcasted_iota(jnp.int32, (2 * seq, 128), 0), seq)
              >= lax.broadcasted_iota(jnp.int32, (2 * seq, 128), 1))
    pairs = CH // 128

    def spread(tile, upper):
        if upper:
            hi = jnp.where(low, 0.0, tile)
            lo = pltpu.roll(hi, head, 1)
        else:
            lo = jnp.where(low, tile, 0.0)
            hi = pltpu.roll(lo, head, 1)
        return jnp.concatenate([lo, hi], axis=0).astype(BF16)

    for b in range(per):
        own_in[b].wait()
        if n_dev > 1:
            for k in order:
                send_in(k, b).wait_recv()
        rb = pl.ds(b * seq, seq)
        normalize(hid, attn_norm, b * seq, seq)
        for i in range(4):
            if b == 0:
                ready(i)
            term = nt_dot(norm[rb, i * CH:(i + 1) * CH], ring[i])
            if i == 0:
                acc[rb, :] = term
            elif i < 3:
                acc[rb, :] += term
            else:
                q[rb, :] = (acc[rb, :] + term).astype(BF16)
            if b == per - 1:
                if i % 2 == 0:
                    cols(wg, 2 + i // 2, i).start()
                else:
                    cols(wu, 2 + i // 2, i).start()
        if b == 0:
            k_load.wait()
            v_load.wait()
        kv[rb, :] = nt_dot(norm[rb, :], kvw[...]).astype(BF16)

        def attend(it, _, rb=rb):
            for m in (2 * it, 2 * it + 1):
                attend_tile(m, rb)
            return 0

        def attend_tile(m, rb):
            kt = kv[rb, pl.ds(pl.multiple_of(m * 128, 128), 128)].astype(F32)
            vt = kv[rb, pl.ds(pl.multiple_of(CH + m * 128, 128), 128)].astype(F32)
            for par in range(2):
                k2 = spread(kt, par)
                v2 = spread(vt, par)
                c0 = pl.multiple_of((2 * m + par) * 256, 128)
                qs = jnp.concatenate([q[rb, pl.ds(c0, 128)], q[rb, pl.ds(c0 + 128, 128)]], axis=0)
                s = nt_dot(qs, k2)
                ps = []
                for h in range(2):
                    sh = jnp.where(causal, s[:, h * 128:(h + 1) * 128] * head ** -0.5, -jnp.inf)
                    e = jnp.exp(sh - jnp.max(sh, axis=-1, keepdims=True))
                    ps.append((e * (1.0 / jnp.sum(e, axis=-1, keepdims=True))).astype(BF16))
                o = nn_dot(jnp.concatenate(ps, axis=1), v2).astype(BF16)
                norm[rb, pl.ds(c0, 128)] = o[:seq]
                norm[rb, pl.ds(c0 + 128, 128)] = o[seq:]

        lax.fori_loop(0, pairs // 2, attend, 0)

    def out_proj(n, _):
        ready(4 + n)
        c = pl.ds(pl.multiple_of(n * CH, CH), CH)
        h1 = (hid[:, c].astype(F32) + nn_dot(norm[...], ring[4 + n])).astype(BF16)
        res[:, c] = h1
        acc[:, c] = h1.astype(F32)
        block(wd, 1, n, 4 + n).start()
        return 0

    lax.fori_loop(0, 4, out_proj, 0)

    normalize(res, mlp_norm)

    def up(i, s):
        slots = [slot_of(4 * i + p) for p in range(4)]
        for sl in slots:
            ready(sl)
        for p in range(2):
            gate = nn_dot(norm[...], ring[slots[2 * p]])
            upv = nn_dot(norm[...], ring[slots[2 * p + 1]])
            act[:, pl.ds(pl.multiple_of((2 * i + p) * CH, CH), CH)] = (silu(gate) * upv).astype(BF16)

        @pl.when(s < 3)
        def _():
            for p in range(2):
                cols(wg, 4 * (s + 1) + 2 * i + p, slots[2 * p]).start()
                cols(wu, 4 * (s + 1) + 2 * i + p, slots[2 * p + 1]).start()

        @pl.when(s == 3)
        def _():
            for p in range(4):
                cols(wix, 4 * i + p, slots[p]).start()

        return s

    lax.fori_loop(0, 2, up, jnp.int32(0))
    for n in range(4):
        first_down(n).wait()
    for n in range(4):
        acc[:, n * CH:(n + 1) * CH] += nn_dot(act[...], early[n][...])

    def mlp(s, _):
        lax.fori_loop(0, 2, up, s)
        for n in range(4):
            ready((16 + n) % NS)
        for n in range(4):
            acc[:, n * CH:(n + 1) * CH] += nn_dot(act[...], ring[(16 + n) % NS])

        @pl.when(s < 3)
        def _():
            for n in range(4):
                block(wd, s + 1, n, (16 + n) % NS).start()

        @pl.when(s == 3)
        def _():
            for n in range(4):
                cols(wiz, n, (16 + n) % NS).start()

        return 0

    lax.fori_loop(1, 4, mlp, 0)

    normalize(acc, mamba_norm, 0, rows, res)
    pitch = seq + 8
    tiles = CH // 128
    for i in range(2):
        for b in range(per * tiles):
            xpad[i, pl.ds(b * pitch, 8), :] = jnp.zeros((8, 128), F32)

    def conv_chunk(e):
        i = lax.rem(e, 2)
        whole = conv_b[pl.ds(pl.multiple_of(e * CH, CH), CH)].astype(F32).reshape(1, CH)
        for j in range(tiles):
            c = pl.ds(pl.multiple_of(e * CH + j * 128, 128), 128)
            bias = whole[:, j * 128:(j + 1) * 128]
            taps = [conv_w[k:k + 1, c].astype(F32) for k in range(CONV)]
            for b in range(per):
                v = bias
                for k in range(CONV):
                    v = v + xpad[i, pl.ds((j * per + b) * pitch + 8 - (CONV - 1) + k, seq), :] * taps[k]
                conv[piece(e, b), j * 128:(j + 1) * 128] = silu(v).astype(BF16)

    def inx(e, _):
        sl = slot_of(e)
        ready(sl)
        conv_chunk(jnp.maximum(e - 1, 0))
        xi = nn_dot(norm[...], ring[sl]).astype(BF16).astype(F32)
        for j in range(tiles):
            for b in range(per):
                xpad[lax.rem(e, 2), pl.ds((j * per + b) * pitch + 8, seq), :] = (
                    xi[b * seq:(b + 1) * seq, j * 128:(j + 1) * 128])

        @pl.when(e < 4)
        def _():
            cols(wiz, 4 + e, sl).start()

        @pl.when(e >= 4)
        def _():
            block(wout, lax.rem(e, 2), lax.div(e - 4, 2), sl).start()

        return 0

    lax.fori_loop(0, chunks, inx, 0)
    conv_chunk(jnp.int32(chunks - 1))

    xp_load.wait()
    dt_load.wait()
    r = nt_dot(jnp.concatenate([conv[e * rows:(e + 1) * rows, :] for e in range(chunks)], axis=1), xpw[...])
    dt_in = (rms(r[:, :rank]) * dt_norm[...].reshape(1, rank)).astype(BF16)
    bm = rms(r[:, rank:rank + n_state]) * b_norm[...].reshape(1, n_state)
    cm = rms(r[:, rank + n_state:rank + 2 * n_state]) * c_norm[...].reshape(1, n_state)
    for n in range(n_state):
        bc[n] = jnp.broadcast_to(bm[:, n:n + 1], (rows, 128))
        bc[n_state + n] = jnp.broadcast_to(cm[:, n:n + 1], (rows, 128))
    kv[:, :rank] = dt_in

    def deltas(e, _):
        c = pl.ds(pl.multiple_of(e * CH, CH), CH)
        step = softplus(nn_dot(kv[:, :rank], dtw[:, c]) + dt_bias[c].reshape(1, CH))
        prod = step * conv[pl.ds(pl.multiple_of(e * rows, rows), rows), :].astype(F32)
        for j in range(tiles):
            at = pl.ds((e * tiles + j) * ST, rows)
            dl[at, :] = step[:, j * 128:(j + 1) * 128]
            dc[at, :] = prod[:, j * 128:(j + 1) * 128]
        sl = slot_of(8 + e)
        ready(sl)
        zg[pl.ds(pl.multiple_of(e * rows, rows), rows), :] = nn_dot(norm[...], ring[sl]).astype(BF16)

        @pl.when(e < 4)
        def _():
            block(wout, lax.rem(e, 2), 2 + lax.div(e, 2), sl).start()

        return 0

    lax.fori_loop(0, chunks, deltas, 0)

    def chunk_cols(n):
        return pl.ds(n * CH, CH) if isinstance(n, int) else pl.ds(pl.multiple_of(n * CH, CH), CH)

    def send_out(k, b, n):
        to = peer_of(k)
        return pltpu.make_async_remote_copy(
            src_ref=q.at[pl.ds(pl.multiple_of(b * seq + to * tok, tok), tok), chunk_cols(n)],
            dst_ref=out.at[me * per + b, :, chunk_cols(n)],
            send_sem=out_send,
            recv_sem=out_recv,
            device_id={axis: to},
            device_id_type=pl.DeviceIdType.MESH,
        )

    def own_out(b, n):
        return pltpu.make_async_copy(
            q.at[pl.ds(pl.multiple_of(b * seq + me * tok, tok), tok), chunk_cols(n)],
            out.at[me * per + b, :, chunk_cols(n)],
            own_sem.at[b, n],
        )

    n_part = 4
    part = seq // n_part
    deep = inner // n_part

    def send_chunk(b, n):
        own_out(b, n).start()
        if n_dev > 1:
            for k in order:
                send_out(k, b, n).start()

    def out_matmul(blk, i):
        lhs = jnp.concatenate([zg[piece(i * (deep // CH) + p, 0), :] for p in range(deep // CH)], axis=1)
        to = pl.ds(pl.multiple_of(blk * CH, CH), CH)
        at = pl.ds(pl.multiple_of(lax.rem(i, 2) * deep, deep), deep)
        acc[:seq, to] += nn_dot(lhs, ring[slot_of(4 + 2 * blk + lax.div(i, 2)), at, :])

    for b in range(per):
        rb = pl.ds(b * seq, seq)

        def scan_block(blk, _, b=b, rb=rb):
            base = blk * (8 * ST) + b * seq
            a_rows = [amat[pl.ds(n * SA + blk * 8, 8), :] for n in range(n_state)]
            if b == 1:
                ready(slot_of(4 + 2 * blk))
                ready(slot_of(5 + 2 * blk))

            def step(t, hs):
                at = pl.ds(base + t, 8, stride=ST)
                d = dl[at, :]
                x = dc[at, :]
                new = []
                y = None
                for n in range(n_state):
                    bv = jnp.broadcast_to(bc[n, pl.ds(b * seq + t, 1), :], (8, 128))
                    cv = jnp.broadcast_to(bc[n_state + n, pl.ds(b * seq + t, 1), :], (8, 128))
                    hn = jnp.exp2(d * a_rows[n]) * hs[n] + x * bv
                    new.append(hn)
                    y = hn * cv if y is None else y + hn * cv
                ys[pl.ds(t, 8, stride=seq + 4), :] = y
                return tuple(new)

            def scan_part(i, hs):
                out_matmul(blk, i)
                for u in range(part):
                    hs = step(i * part + u, hs)
                return hs

            zero = tuple(jnp.zeros((8, 128), F32) for _ in range(n_state))
            if b == 1:
                lax.fori_loop(0, n_part, scan_part, zero)
            else:
                lax.fori_loop(0, seq, step, zero, unroll=8)
            if b == 1:
                c = pl.ds(pl.multiple_of(blk * CH, CH), CH)
                q[:seq, c] = acc[:seq, c].astype(BF16)
            for j in range(8):
                c = pl.ds(pl.multiple_of(blk * 1024 + j * 128, 128), 128)
                at = (piece(2 * blk + j // tiles, b), slice(j % tiles * 128, (j % tiles + 1) * 128))
                y = ys[pl.ds(j * (seq + 4), seq), :] + d_skip[c].reshape(1, 128) * conv[at].astype(F32)
                zg[at] = (y * silu(zg[at].astype(F32))).astype(BF16)
            if b == 1:
                send_chunk(0, blk)
            return 0

        lax.fori_loop(0, inner // 1024, scan_block, 0)

    last = per - 1
    rb = pl.ds(last * seq, seq)
    lhs = [zg[piece(e, last), :] for e in range(chunks)]
    for n in range(dim // CH):
        s0 = (4 + 2 * n + 8) % NS
        s1 = (5 + 2 * n + 8) % NS
        c = slice(n * CH, (n + 1) * CH)
        y = (nn_dot(jnp.concatenate(lhs[:chunks // 2], axis=1), ring[s0])
             + nn_dot(jnp.concatenate(lhs[chunks // 2:], axis=1), ring[s1]))
        q[rb, c] = (res[rb, c].astype(F32) + y).astype(BF16)
        send_chunk(last, n)

    for b in range(per):
        for n in range(dim // CH):
            own_out(b, n).wait()
    if n_dev > 1:
        for b in range(per):
            for k in order:
                send_in(k, b).wait_send()
        everything = pltpu.make_async_remote_copy(
            src_ref=out.at[pl.ds(0, n_batch - per)],
            dst_ref=out.at[pl.ds(0, n_batch - per)],
            send_sem=out_send,
            recv_sem=out_recv,
            device_id={axis: peer_of(1)},
            device_id_type=pl.DeviceIdType.MESH,
        )
        everything.wait_send()
        everything.wait_recv()


def local_layers(n_dev, axis, hidden, attn_norm, w_q, w_k, w_v, w_o, mlp_norm, w_gate, w_up, w_down, mamba_norm,
                 w_in_x, w_in_z, conv_w, conv_b, w_xproj, dt_norm, b_norm, c_norm, w_dt, dt_bias, a_log, d_skip, w_out):
    n_batch, tok, dim = hidden.shape
    rows = n_batch * tok
    inner, n_state = a_log.shape
    wq_t = w_q.transpose(1, 2, 0).reshape(-1, dim)
    wk_t = w_k.transpose(1, 2, 0).reshape(-1, dim)
    wv_t = w_v.transpose(1, 2, 0).reshape(-1, dim)
    kv_dim = wk_t.shape[0]
    wo = w_o.reshape(-1, dim)
    wxp = w_xproj.T
    vm = pl.BlockSpec(memory_space=pltpu.VMEM)
    hbm = pl.BlockSpec(memory_space=pl.ANY)
    peers = max(n_dev - 1, 1)
    per = n_batch // n_dev
    lanes = inner // 128
    params = dict(vmem_limit_bytes=63 * 1024 * 1024)
    if n_dev > 1:
        params.update(collective_id=0, has_side_effects=True)
    return pl.pallas_call(
        functools.partial(layer_kernel, n_dev, axis),
        out_shape=jax.ShapeDtypeStruct(hidden.shape, BF16),
        in_specs=[hbm] + [vm] * 11 + [hbm] * 12,
        out_specs=hbm,
        scratch_shapes=[
            pltpu.VMEM((NS, dim, CH), BF16),
            pltpu.VMEM((2 * kv_dim, dim), BF16),
            pltpu.VMEM(wxp.shape, BF16),
            pltpu.VMEM(w_dt.shape, BF16),
            pltpu.VMEM((rows, dim), BF16),
            pltpu.VMEM((rows, dim), BF16),
            pltpu.VMEM((rows, dim), BF16),
            pltpu.VMEM((rows, 2 * kv_dim), BF16),
            pltpu.VMEM((rows, dim), F32),
            pltpu.VMEM((rows, dim), BF16),
            pltpu.VMEM((2, (rows + 8 * per) * (CH // 128), 128), F32),
            pltpu.VMEM((dim, CH), BF16),
            pltpu.VMEM((dim, CH), BF16),
            pltpu.VMEM((2 * n_state, rows, 128), F32),
            pltpu.VMEM((lanes * ST, 128), F32),
            pltpu.VMEM((lanes * ST, 128), F32),
            pltpu.VMEM((8 * (rows // per + 4), 128), F32),
            pltpu.VMEM((n_state * SA, 128), F32),
            pltpu.VMEM((2, dim, CH), BF16),
            pltpu.SemaphoreType.DMA((NS,)),
            pltpu.SemaphoreType.DMA((4,)),
            pltpu.SemaphoreType.DMA((4,)),
            pltpu.SemaphoreType.DMA((peers, per)),
            pltpu.SemaphoreType.DMA((peers, per)),
            pltpu.SemaphoreType.DMA,
            pltpu.SemaphoreType.DMA,
            pltpu.SemaphoreType.DMA((per, dim // CH + 1)),
        ],
        compiler_params=pltpu.CompilerParams(**params),
        cost_estimate=pl.CostEstimate(flops=45_000_000_000, bytes_accessed=180_000_000, transcendentals=20_000_000),
        name="layers",
    )(hidden, attn_norm, mlp_norm, mamba_norm, conv_w, conv_b, dt_norm, b_norm, c_norm, dt_bias, d_skip, a_log.T,
      wq_t, wk_t, wv_t, wo, w_gate, w_up, w_down, w_in_x, w_in_z, wxp, w_dt, w_out)


def solution(mesh):
    act_spec = P("dp", "sp", None)
    return jax.shard_map(
        functools.partial(local_layers, mesh.shape["sp"], "sp"),
        mesh=mesh,
        in_specs=(act_spec,) + (P(),) * 23,
        out_specs=act_spec,
        check_vma=False,
    )
```

```python
import functools
import math

import jax
import jax.numpy as jnp
from jax import lax
from jax.experimental import pallas as pl
from jax.experimental.pallas import tpu as pltpu
from jax.sharding import PartitionSpec as P

EPS = 1e-6
CONV = 4
CH = 512
NS = 12
ST = 260
SA = 33
LOG2E = math.log2(math.e)
F32 = jnp.float32
BF16 = jnp.bfloat16


def nt_dot(a, b):
    return lax.dot_general(a, b, (((1,), (1,)), ((), ())), preferred_element_type=F32)


def nn_dot(a, b):
    return jnp.dot(a, b, preferred_element_type=F32)


def silu(v):
    return v * (1.0 / (1.0 + jnp.exp(-v)))


def softplus(v):
    return jnp.maximum(v, 0.0) + jnp.log1p(jnp.exp(-jnp.abs(v)))


def rms(v):
    return v * lax.rsqrt(jnp.mean(v * v, axis=-1, keepdims=True) + EPS)


def layer_kernel(
    n_dev, axis, x_in, attn_norm, mlp_norm, mamba_norm, conv_w, conv_b, dt_norm, b_norm, c_norm, dt_bias, d_skip, alog,
    wq, wk, wv, wo, wg, wu, wd, wix, wiz, wxp, wdt, wout,
    out, ring, kvw, xpw, dtw, hid, norm, q, kv, acc, res, xpad, conv, zg, bc, dl, dc, ys, amat,
    spare, sem, sem2, sem3, in_send, in_recv, out_send, out_recv, own_sem,
):
    n_batch, tok, dim = x_in.shape
    per = n_batch // n_dev
    seq = tok * n_dev
    rows = per * seq
    inner = wix.shape[1]
    chunks = inner // CH
    n_state = alog.shape[0]
    rank = wdt.shape[0]
    me = lax.axis_index(axis) if n_dev > 1 else 0
    act = q

    def peer_of(k):
        chips = n_dev // 2
        chip = lax.rem(lax.div(me, 2) + k // 2, chips)
        return chip * 2 + lax.rem(lax.rem(me, 2) + k % 2, 2)

    order = sorted(range(1, n_dev), key=lambda k: (-min(k // 2, n_dev // 2 - k // 2), k % 2, k))

    def cols(w, c, slot):
        return pltpu.make_async_copy(w.at[:, pl.ds(c * CH, CH)], ring.at[slot], sem.at[slot])

    def block(w, k, c, slot):
        return pltpu.make_async_copy(w.at[pl.ds(k * dim, dim), pl.ds(c * CH, CH)], ring.at[slot], sem.at[slot])

    early = [spare.at[0], spare.at[1], conv, zg]

    def first_down(n):
        return pltpu.make_async_copy(wd.at[pl.ds(0, dim), pl.ds(n * CH, CH)], early[n], sem3.at[n])

    def piece(e, b):
        return pl.ds(pl.multiple_of(e * rows + b * seq, seq), seq)

    def ready(slot):
        pltpu.make_async_copy(wg.at[:, pl.ds(0, CH)], ring.at[slot], sem.at[slot]).wait()

    def slot_of(p):
        return lax.rem(p + 8, NS)

    def send_in(k, b):
        to = peer_of(k)
        return pltpu.make_async_remote_copy(
            src_ref=x_in.at[to * per + b],
            dst_ref=hid.at[pl.ds(pl.multiple_of(b * seq + me * tok, tok), tok)],
            send_sem=in_send.at[k - 1, b],
            recv_sem=in_recv.at[k - 1, b],
            device_id={axis: to},
            device_id_type=pl.DeviceIdType.MESH,
        )

    own_in = [
        pltpu.make_async_copy(
            x_in.at[me * per + b],
            hid.at[pl.ds(pl.multiple_of(b * seq + me * tok, tok), tok)],
            own_sem.at[b, dim // CH],
        )
        for b in range(per)
    ]

    k_load = pltpu.make_async_copy(wk, kvw.at[pl.ds(0, CH)], sem2.at[0])
    v_load = pltpu.make_async_copy(wv, kvw.at[pl.ds(CH, CH)], sem2.at[1])
    xp_load = pltpu.make_async_copy(wxp, xpw, sem2.at[2])
    dt_load = pltpu.make_async_copy(wdt, dtw, sem2.at[3])
    for copy in own_in:
        copy.start()
    if n_dev > 1:
        barrier = pltpu.get_barrier_semaphore()
        for k in range(1, n_dev):
            pl.semaphore_signal(barrier, inc=1, device_id={axis: peer_of(k)}, device_id_type=pl.DeviceIdType.MESH)
    for i in range(4):
        cols(wq, i, i).start()
    k_load.start()
    v_load.start()
    if n_dev > 1:
        pl.semaphore_wait(barrier, n_dev - 1)
        for b in range(per):
            for k in order:
                send_in(k, b).start()
    for i in range(4):
        cols(wo, i, 4 + i).start()
    cols(wg, 0, 8).start()
    cols(wu, 0, 9).start()
    cols(wg, 1, 10).start()
    cols(wu, 1, 11).start()
    for n in range(4):
        first_down(n).start()
    xp_load.start()
    dt_load.start()

    def normalize(src, gain_ref, start=0, count=rows, keep=None):
        gain = gain_ref[...].astype(F32).reshape(1, dim)

        def body(i, _):
            r = pl.ds(pl.multiple_of(start + i * 16, 16), 16)
            v = src[r, :]
            if keep is not None:
                v = v.astype(BF16)
                keep[r, :] = v
            v = v.astype(F32)
            if keep is not None:
                src[r, :] = v
            norm[r, :] = (rms(v) * gain).astype(BF16)
            return 0

        lax.fori_loop(0, count // 16, body, 0, unroll=2)

    for j in range(inner // 128):
        a = -jnp.exp(alog[:, j * 128:(j + 1) * 128]) * LOG2E
        amat[pl.ds(j, n_state, stride=SA), :] = a

    head = 64
    lane = lax.broadcasted_iota(jnp.int32, (seq, 128), 1)
    low = lane < head
    causal = (lax.rem(lax.broadcasted_iota(jnp.int32, (2 * seq, 128), 0), seq)
              >= lax.broadcasted_iota(jnp.int32, (2 * seq, 128), 1))
    pairs = CH // 128

    def spread(tile, upper):
        if upper:
            hi = jnp.where(low, 0.0, tile)
            lo = pltpu.roll(hi, head, 1)
        else:
            lo = jnp.where(low, tile, 0.0)
            hi = pltpu.roll(lo, head, 1)
        return jnp.concatenate([lo, hi], axis=0).astype(BF16)

    for b in range(per):
        own_in[b].wait()
        if n_dev > 1:
            for k in order:
                send_in(k, b).wait_recv()
        rb = pl.ds(b * seq, seq)
        normalize(hid, attn_norm, b * seq, seq)
        for i in range(4):
            if b == 0:
                ready(i)
            term = nt_dot(norm[rb, i * CH:(i + 1) * CH], ring[i])
            if i == 0:
                acc[rb, :] = term
            elif i < 3:
                acc[rb, :] += term
            else:
                q[rb, :] = (acc[rb, :] + term).astype(BF16)
            if b == per - 1:
                if i % 2 == 0:
                    cols(wg, 2 + i // 2, i).start()
                else:
                    cols(wu, 2 + i // 2, i).start()
        if b == 0:
            k_load.wait()
            v_load.wait()
        kv[rb, :] = nt_dot(norm[rb, :], kvw[...]).astype(BF16)

        def attend(it, _, rb=rb):
            for m in (2 * it, 2 * it + 1):
                attend_tile(m, rb)
            return 0

        def attend_tile(m, rb):
            kt = kv[rb, pl.ds(pl.multiple_of(m * 128, 128), 128)].astype(F32)
            vt = kv[rb, pl.ds(pl.multiple_of(CH + m * 128, 128), 128)].astype(F32)
            for par in range(2):
                k2 = spread(kt, par)
                v2 = spread(vt, par)
                c0 = pl.multiple_of((2 * m + par) * 256, 128)
                qs = jnp.concatenate([q[rb, pl.ds(c0, 128)], q[rb, pl.ds(c0 + 128, 128)]], axis=0)
                s = nt_dot(qs, k2)
                ps = []
                for h in range(2):
                    sh = jnp.where(causal, s[:, h * 128:(h + 1) * 128] * head ** -0.5, -jnp.inf)
                    e = jnp.exp(sh - jnp.max(sh, axis=-1, keepdims=True))
                    ps.append((e * (1.0 / jnp.sum(e, axis=-1, keepdims=True))).astype(BF16))
                o = nn_dot(jnp.concatenate(ps, axis=1), v2).astype(BF16)
                norm[rb, pl.ds(c0, 128)] = o[:seq]
                norm[rb, pl.ds(c0 + 128, 128)] = o[seq:]

        lax.fori_loop(0, pairs // 2, attend, 0)

    def out_proj(n, _):
        ready(4 + n)
        c = pl.ds(pl.multiple_of(n * CH, CH), CH)
        h1 = (hid[:, c].astype(F32) + nn_dot(norm[...], ring[4 + n])).astype(BF16)
        res[:, c] = h1
        acc[:, c] = h1.astype(F32)
        block(wd, 1, n, 4 + n).start()
        return 0

    lax.fori_loop(0, 4, out_proj, 0)

    normalize(res, mlp_norm)

    def up(i, s):
        slots = [slot_of(4 * i + p) for p in range(4)]
        for sl in slots:
            ready(sl)
        for p in range(2):
            gate = nn_dot(norm[...], ring[slots[2 * p]])
            upv = nn_dot(norm[...], ring[slots[2 * p + 1]])
            act[:, pl.ds(pl.multiple_of((2 * i + p) * CH, CH), CH)] = (silu(gate) * upv).astype(BF16)

        @pl.when(s < 3)
        def _():
            for p in range(2):
                cols(wg, 4 * (s + 1) + 2 * i + p, slots[2 * p]).start()
                cols(wu, 4 * (s + 1) + 2 * i + p, slots[2 * p + 1]).start()

        @pl.when(s == 3)
        def _():
            for p in range(4):
                cols(wix, 4 * i + p, slots[p]).start()

        return s

    lax.fori_loop(0, 2, up, jnp.int32(0))
    for n in range(4):
        first_down(n).wait()
    for n in range(4):
        acc[:, n * CH:(n + 1) * CH] += nn_dot(act[...], early[n][...])

    def mlp(s, _):
        lax.fori_loop(0, 2, up, s)
        for n in range(4):
            ready((16 + n) % NS)
        for n in range(4):
            acc[:, n * CH:(n + 1) * CH] += nn_dot(act[...], ring[(16 + n) % NS])

        @pl.when(s < 3)
        def _():
            for n in range(4):
                block(wd, s + 1, n, (16 + n) % NS).start()

        @pl.when(s == 3)
        def _():
            for n in range(4):
                cols(wiz, n, (16 + n) % NS).start()

        return 0

    lax.fori_loop(1, 4, mlp, 0)

    normalize(acc, mamba_norm, 0, rows, res)
    pitch = seq + 8
    tiles = CH // 128
    for i in range(2):
        for b in range(per * tiles):
            xpad[i, pl.ds(b * pitch, 8), :] = jnp.zeros((8, 128), F32)

    def conv_chunk(e, i):
        whole = conv_b[pl.ds(pl.multiple_of(e * CH, CH), CH)].astype(F32).reshape(1, CH)
        for j in range(tiles):
            c = pl.ds(pl.multiple_of(e * CH + j * 128, 128), 128)
            bias = whole[:, j * 128:(j + 1) * 128]
            taps = [conv_w[k:k + 1, c].astype(F32) for k in range(CONV)]
            for b in range(per):
                v = bias
                for k in range(CONV):
                    v = v + xpad[i, pl.ds((j * per + b) * pitch + 8 - (CONV - 1) + k, seq), :] * taps[k]
                conv[piece(e, b), j * 128:(j + 1) * 128] = silu(v).astype(BF16)

    def in_matmul(sl):
        return nn_dot(norm[...], ring[sl]).astype(BF16).astype(F32)

    def keep_xi(i, xi):
        for j in range(tiles):
            for b in range(per):
                xpad[i, pl.ds((j * per + b) * pitch + 8, seq), :] = xi[b * seq:(b + 1) * seq, j * 128:(j + 1) * 128]

    def inx(p, _):
        s0 = slot_of(2 * p)
        s1 = slot_of(2 * p + 1)
        ready(s0)
        ready(s1)
        conv_chunk(jnp.maximum(2 * p - 1, 0), 1)
        keep_xi(0, in_matmul(s0))
        xi = in_matmul(s1)
        conv_chunk(2 * p, 0)
        keep_xi(1, xi)

        @pl.when(p < 2)
        def _():
            cols(wiz, 4 + 2 * p, s0).start()
            cols(wiz, 5 + 2 * p, s1).start()

        @pl.when(p >= 2)
        def _():
            block(wout, 0, p - 2, s0).start()
            block(wout, 1, p - 2, s1).start()

        return 0

    lax.fori_loop(0, chunks // 2, inx, 0)
    conv_chunk(jnp.int32(chunks - 1), 1)

    xp_load.wait()
    dt_load.wait()
    r = nt_dot(jnp.concatenate([conv[e * rows:(e + 1) * rows, :] for e in range(chunks)], axis=1), xpw[...])
    dt_in = (rms(r[:, :rank]) * dt_norm[...].reshape(1, rank)).astype(BF16)
    bm = rms(r[:, rank:rank + n_state]) * b_norm[...].reshape(1, n_state)
    cm = rms(r[:, rank + n_state:rank + 2 * n_state]) * c_norm[...].reshape(1, n_state)
    kv[:, :rank] = dt_in
    per_pair = 2 * n_state // chunks

    def deltas(e):
        c = slice(e * CH, (e + 1) * CH)
        step = softplus(nn_dot(kv[:, :rank], dtw[:, c]) + dt_bias[c].reshape(1, CH))
        prod = step * conv[e * rows:(e + 1) * rows, :].astype(F32)
        for j in range(tiles):
            at = pl.ds((e * tiles + j) * ST, rows)
            dl[at, :] = step[:, j * 128:(j + 1) * 128]
            dc[at, :] = prod[:, j * 128:(j + 1) * 128]

    for p in range(chunks // 2):
        slots = [(16 + 2 * p + k) % NS for k in range(2)]
        for sl in slots:
            ready(sl)
        for k in range(2):
            e = 2 * p + k
            zg[e * rows:(e + 1) * rows, :] = nn_dot(norm[...], ring[slots[k]]).astype(BF16)
            deltas(e)
        for n in range(p * per_pair, (p + 1) * per_pair):
            bc[n] = jnp.broadcast_to(bm[:, n:n + 1], (rows, 128))
            bc[n_state + n] = jnp.broadcast_to(cm[:, n:n + 1], (rows, 128))
        if p < 2:
            for k in range(2):
                block(wout, k, 2 + p, slots[k]).start()

    def chunk_cols(n):
        return pl.ds(n * CH, CH) if isinstance(n, int) else pl.ds(pl.multiple_of(n * CH, CH), CH)

    def send_out(k, b, n):
        to = peer_of(k)
        return pltpu.make_async_remote_copy(
            src_ref=q.at[pl.ds(pl.multiple_of(b * seq + to * tok, tok), tok), chunk_cols(n)],
            dst_ref=out.at[me * per + b, :, chunk_cols(n)],
            send_sem=out_send,
            recv_sem=out_recv,
            device_id={axis: to},
            device_id_type=pl.DeviceIdType.MESH,
        )

    def own_out(b, n):
        return pltpu.make_async_copy(
            q.at[pl.ds(pl.multiple_of(b * seq + me * tok, tok), tok), chunk_cols(n)],
            out.at[me * per + b, :, chunk_cols(n)],
            own_sem.at[b, n],
        )

    n_part = 4
    part = seq // n_part
    deep = inner // n_part

    def send_chunk(b, n):
        own_out(b, n).start()
        if n_dev > 1:
            for k in order:
                send_out(k, b, n).start()

    def out_matmul(blk, i):
        lhs = jnp.concatenate([zg[piece(i * (deep // CH) + p, 0), :] for p in range(deep // CH)], axis=1)
        to = pl.ds(pl.multiple_of(blk * CH, CH), CH)
        at = pl.ds(pl.multiple_of(lax.rem(i, 2) * deep, deep), deep)
        acc[:seq, to] += nn_dot(lhs, ring[slot_of(4 + 2 * blk + lax.div(i, 2)), at, :])

    for b in range(per):
        rb = pl.ds(b * seq, seq)

        def scan_block(blk, _, b=b, rb=rb):
            base = blk * (8 * ST) + b * seq
            a_rows = [amat[pl.ds(n * SA + blk * 8, 8), :] for n in range(n_state)]
            if b == 1:
                ready(slot_of(4 + 2 * blk))
                ready(slot_of(5 + 2 * blk))

            def step(t, hs):
                at = pl.ds(base + t, 8, stride=ST)
                d = dl[at, :]
                x = dc[at, :]
                new = []
                y = None
                for n in range(n_state):
                    bv = jnp.broadcast_to(bc[n, pl.ds(b * seq + t, 1), :], (8, 128))
                    cv = jnp.broadcast_to(bc[n_state + n, pl.ds(b * seq + t, 1), :], (8, 128))
                    hn = jnp.exp2(d * a_rows[n]) * hs[n] + x * bv
                    new.append(hn)
                    y = hn * cv if y is None else y + hn * cv
                ys[pl.ds(t, 8, stride=seq + 4), :] = y
                return tuple(new)

            def scan_part(i, hs):
                out_matmul(blk, i)
                for u in range(part):
                    hs = step(i * part + u, hs)
                return hs

            zero = tuple(jnp.zeros((8, 128), F32) for _ in range(n_state))
            if b == 1:
                lax.fori_loop(0, n_part, scan_part, zero)
            else:
                lax.fori_loop(0, seq, step, zero, unroll=8)
            if b == 1:
                c = pl.ds(pl.multiple_of(blk * CH, CH), CH)
                q[:seq, c] = acc[:seq, c].astype(BF16)
            for j in range(8):
                c = pl.ds(pl.multiple_of(blk * 1024 + j * 128, 128), 128)
                at = (piece(2 * blk + j // tiles, b), slice(j % tiles * 128, (j % tiles + 1) * 128))
                y = ys[pl.ds(j * (seq + 4), seq), :] + d_skip[c].reshape(1, 128) * conv[at].astype(F32)
                zg[at] = (y * silu(zg[at].astype(F32))).astype(BF16)
            if b == 1:
                send_chunk(0, blk)
            return 0

        lax.fori_loop(0, inner // 1024, scan_block, 0)

    last = per - 1
    rb = pl.ds(last * seq, seq)
    lhs = [zg[piece(e, last), :] for e in range(chunks)]
    for n in range(dim // CH):
        s0 = (4 + 2 * n + 8) % NS
        s1 = (5 + 2 * n + 8) % NS
        c = slice(n * CH, (n + 1) * CH)
        y = (nn_dot(jnp.concatenate(lhs[:chunks // 2], axis=1), ring[s0])
             + nn_dot(jnp.concatenate(lhs[chunks // 2:], axis=1), ring[s1]))
        q[rb, c] = (res[rb, c].astype(F32) + y).astype(BF16)
        send_chunk(last, n)

    for b in range(per):
        for n in range(dim // CH):
            own_out(b, n).wait()
    if n_dev > 1:
        for b in range(per):
            for k in order:
                send_in(k, b).wait_send()
        everything = pltpu.make_async_remote_copy(
            src_ref=out.at[pl.ds(0, n_batch - per)],
            dst_ref=out.at[pl.ds(0, n_batch - per)],
            send_sem=out_send,
            recv_sem=out_recv,
            device_id={axis: peer_of(1)},
            device_id_type=pl.DeviceIdType.MESH,
        )
        everything.wait_send()
        everything.wait_recv()


def local_layers(n_dev, axis, hidden, attn_norm, w_q, w_k, w_v, w_o, mlp_norm, w_gate, w_up, w_down, mamba_norm,
                 w_in_x, w_in_z, conv_w, conv_b, w_xproj, dt_norm, b_norm, c_norm, w_dt, dt_bias, a_log, d_skip, w_out):
    n_batch, tok, dim = hidden.shape
    rows = n_batch * tok
    inner, n_state = a_log.shape
    wq_t = w_q.transpose(1, 2, 0).reshape(-1, dim)
    wk_t = w_k.transpose(1, 2, 0).reshape(-1, dim)
    wv_t = w_v.transpose(1, 2, 0).reshape(-1, dim)
    kv_dim = wk_t.shape[0]
    wo = w_o.reshape(-1, dim)
    wxp = w_xproj.T
    vm = pl.BlockSpec(memory_space=pltpu.VMEM)
    hbm = pl.BlockSpec(memory_space=pl.ANY)
    peers = max(n_dev - 1, 1)
    per = n_batch // n_dev
    lanes = inner // 128
    params = dict(vmem_limit_bytes=63 * 1024 * 1024)
    if n_dev > 1:
        params.update(collective_id=0, has_side_effects=True)
    return pl.pallas_call(
        functools.partial(layer_kernel, n_dev, axis),
        out_shape=jax.ShapeDtypeStruct(hidden.shape, BF16),
        in_specs=[hbm] + [vm] * 11 + [hbm] * 12,
        out_specs=hbm,
        scratch_shapes=[
            pltpu.VMEM((NS, dim, CH), BF16),
            pltpu.VMEM((2 * kv_dim, dim), BF16),
            pltpu.VMEM(wxp.shape, BF16),
            pltpu.VMEM(w_dt.shape, BF16),
            pltpu.VMEM((rows, dim), BF16),
            pltpu.VMEM((rows, dim), BF16),
            pltpu.VMEM((rows, dim), BF16),
            pltpu.VMEM((rows, 2 * kv_dim), BF16),
            pltpu.VMEM((rows, dim), F32),
            pltpu.VMEM((rows, dim), BF16),
            pltpu.VMEM((2, (rows + 8 * per) * (CH // 128), 128), F32),
            pltpu.VMEM((dim, CH), BF16),
            pltpu.VMEM((dim, CH), BF16),
            pltpu.VMEM((2 * n_state, rows, 128), F32),
            pltpu.VMEM((lanes * ST, 128), F32),
            pltpu.VMEM((lanes * ST, 128), F32),
            pltpu.VMEM((8 * (rows // per + 4), 128), F32),
            pltpu.VMEM((n_state * SA, 128), F32),
            pltpu.VMEM((2, dim, CH), BF16),
            pltpu.SemaphoreType.DMA((NS,)),
            pltpu.SemaphoreType.DMA((4,)),
            pltpu.SemaphoreType.DMA((4,)),
            pltpu.SemaphoreType.DMA((peers, per)),
            pltpu.SemaphoreType.DMA((peers, per)),
            pltpu.SemaphoreType.DMA,
            pltpu.SemaphoreType.DMA,
            pltpu.SemaphoreType.DMA((per, dim // CH + 1)),
        ],
        compiler_params=pltpu.CompilerParams(**params),
        cost_estimate=pl.CostEstimate(flops=45_000_000_000, bytes_accessed=180_000_000, transcendentals=20_000_000),
        name="layers",
    )(hidden, attn_norm, mlp_norm, mamba_norm, conv_w, conv_b, dt_norm, b_norm, c_norm, dt_bias, d_skip, a_log.T,
      wq_t, wk_t, wv_t, wo, w_gate, w_up, w_down, w_in_x, w_in_z, wxp, w_dt, w_out)


def solution(mesh):
    act_spec = P("dp", "sp", None)
    return jax.shard_map(
        functools.partial(local_layers, mesh.shape["sp"], "sp"),
        mesh=mesh,
        in_specs=(act_spec,) + (P(),) * 23,
        out_specs=act_spec,
        check_vma=False,
    )
```
